32 devices in a mesh: chan: 8 (over y, x, core), tm: 4 (over z).
Axes of the slice: x: 2, y: 2, z: 4, core: 2. Of those that a mesh axis runs over, the one named last changes fastest.
Arguments:
- voltages: bfloat16 [2, 8, 2048, 512], P(None, None, 'chan', 'tm'), may hold values from -0.25 to 0.25
- assignment: int32 [1024, 1], replicated, may hold values from 0 to 7; in each aligned block of 1024 rows (0 to 1023, 1024 to 2047, ...) at most 192 rows name the same one
- slot_subarray_index: int32 [8], replicated, may hold values from 0 to 7, each once
Outputs:
- visibilities: float32 [8, 8, 2, 384, 384], P('tm', 'chan')
The draws below stay inside these ranges and needn't reach their ends.
Inputs may be any that keep to these rules, and one draw needn't show every extreme that they name: `assignment`: no subarray holds more than 192 antennas; one holds exactly 192. `slot_subarray_index`: each subarray appears once.
All inputs are finite; a program needn't handle non-finite values.
Results may differ from the reference program's by a relative error of at most 0.008.
Values may be sent and summed in bfloat16 or wider, within the bound.
A program may use at most 64 MiB of HBM per device.

```python
import math
import jax
import jax.numpy as jnp
import numpy as np
from jax import lax

ANTENNA_TOTAL = 1024
SUBARRAY_TOTAL = 8
SAMPLES_LOCAL = 128
INPUTS = 2048
ANTENNA_LIMIT = 192
SLOT = 384
CHANS = 8
SAMPLES = 512
N_TM = 4


def steps_of(key, dims, shards, low, high):
    gain = 1.0
    for axis_at, shards_of in shards:
        steps = jax.random.uniform(jax.random.fold_in(jax.random.fold_in(key, 6), axis_at), (shards_of,), jnp.float32, low / len(shards), high / len(shards))
        gain = gain * jnp.repeat(jnp.exp(steps), dims[axis_at] // shards_of).reshape((-1,) + (1,) * (len(dims) - 1 - axis_at))
    return gain


def deal_out(stream_key, own, number, rows, count, top, bound, slope):
    order = jax.random.permutation(stream_key, count)
    crowded, ordinary = shares(count, rows * top, bound, slope, True), shares(count, rows * top, bound, slope, False)
    places = jnp.arange(count)

    def named(tallies, offset_by):
        used = int((tallies > 0).sum())
        fixed = max(1, used // 4)
        shifted = fixed + (places - fixed + offset_by * (used - fixed)) % max(1, count - fixed)
        return jnp.zeros((count,), jnp.int32).at[order[jnp.where(places < fixed, places, shifted)]].set(jnp.asarray(tallies, jnp.int32))

    tallies = jnp.where(number % 4 == 0, named(crowded, number // 4), named(ordinary, number - number // 4 - 1))
    mixed = jax.random.permutation(jax.random.fold_in(own, 3), count)
    giver, receiver = mixed[0:count // 2 * 2:2], mixed[1:count // 2 * 2:2]
    margin = jnp.minimum(tallies[giver] - 1, bound - tallies[receiver]) // 2
    margin = jnp.where((giver == order[0]) | (receiver == order[0]) | (tallies[receiver] == 0), 0, jnp.maximum(margin, 0))
    shifted = jax.random.randint(jax.random.fold_in(own, 4), (count // 2,), 0, 1 << 20) % (margin + 1)
    tallies = tallies.at[giver].add(-shifted).at[receiver].add(shifted)
    labels = jnp.searchsorted(jnp.cumsum(tallies), jnp.arange(rows * top), side="right").astype(jnp.int32)
    grid = labels.reshape(top, rows).T
    grid = grid[jax.random.permutation(jax.random.fold_in(own, 1), rows)]
    offset_by = jax.random.randint(jax.random.fold_in(own, 2), (rows, 1), 0, top)
    return jnp.take_along_axis(grid, (jnp.arange(top)[None, :] + offset_by) % top, axis=1)


def shares(number_of, total, limit, lean, full):
    weights = [(1 << 20) // math.isqrt(rank ** lean) + 1 for rank in range(1, number_of + 1)]
    largest = limit if full else min(limit, max(-(-total // number_of), total * weights[0] // sum(weights)))
    least = 1 if total - largest >= number_of - 1 else 0
    holding, spare = [largest] + [least] * (number_of - 1), total - largest - least * (number_of - 1)
    while spare > 0:
        free = [i for i in range(1, number_of) if holding[i] < largest] or [i for i in range(1, number_of) if holding[i] < limit]
        mass, remaining = sum([weights[i] for i in free]), spare
        for i in free:
            addition = min(limit - holding[i], max(1, remaining * weights[i] // mass), spare)
            holding[i] = holding[i] + addition
            spare = spare - addition
    return np.array(holding)


def scatter_about(rng, shape, scale, limit, pieces=(), kind=jnp.bfloat16):
    array = jax.random.normal(rng, shape, jnp.float32) * scale
    if len(pieces) > 0:
        array = steps_of(rng, shape, pieces, -0.22, 0.18) * array
    return jnp.clip(array, min=-limit, max=limit).astype(kind)


def setup_inputs(seed: int = 0) -> dict:
    seeds = jax.random.split(jax.random.key(seed), 4)
    voltages = scatter_about(seeds[0], (2, CHANS, INPUTS, SAMPLES), SAMPLES ** -0.5, 0.25, ((2, 8), (3, 4)))
    assignment_keys = jax.random.split(jax.random.fold_in(seeds[1], 1), ANTENNA_TOTAL // ANTENNA_TOTAL)
    assignment_turns = jax.random.permutation(jax.random.fold_in(seeds[1], 3), ANTENNA_TOTAL // ANTENNA_TOTAL)
    assignment = jax.vmap(lambda own, number: deal_out(jax.random.fold_in(seeds[1], 2), own, number, ANTENNA_TOTAL, SUBARRAY_TOTAL, 1, ANTENNA_LIMIT, 2))(assignment_keys, assignment_turns).reshape((ANTENNA_TOTAL, 1))
    slot_subarray_index = jax.random.permutation(seeds[2], SUBARRAY_TOTAL).astype(jnp.int32)
    return {"voltages": voltages, "assignment": assignment, "slot_subarray_index": slot_subarray_index}


def result_slot_lookup(assignment, slot_subarray_index):
    owner = jnp.repeat(assignment[:, 0], 2).astype(jnp.int32)
    onehot = (owner[:, None] == jnp.arange(SUBARRAY_TOTAL, dtype=jnp.int32)[None, :]).astype(jnp.int32)
    ranks = jnp.sum((jnp.cumsum(onehot, axis=0) - onehot) * onehot, axis=1).astype(jnp.int32)
    table = jnp.full((SUBARRAY_TOTAL, SLOT), INPUTS, jnp.int32)
    table = table.at[owner, ranks].set(jnp.arange(INPUTS, dtype=jnp.int32))
    return table[slot_subarray_index.astype(jnp.int32)].reshape(-1).astype(jnp.int32)


def compact(block, rows):
    parts, chans, inputs, samples = block.shape
    padded_voltages = jnp.concatenate([block, jnp.zeros((parts, chans, 1, samples), block.dtype)], axis=2)
    picked = jnp.take(padded_voltages, rows, axis=2)
    picked = picked.reshape(parts, chans, SUBARRAY_TOTAL, SLOT, samples)
    picked = jnp.transpose(picked, (2, 1, 0, 3, 4))
    return picked.reshape(SUBARRAY_TOTAL, chans, 2 * SLOT, samples)


def gram(stacked):
    stacked = stacked.astype(jnp.float32)
    full = jnp.einsum("...pt,...qt->...pq", stacked, stacked)
    half = stacked.shape[-2] // 2
    real = full[..., :half, :half] + full[..., half:, half:]
    imag = full[..., half:, :half] - full[..., :half, half:]
    return jnp.stack([real, imag], axis=-3)


def blocked_gram(stacked):
    total = None
    for block_index in range(N_TM):
        piece = stacked[..., block_index * SAMPLES_LOCAL:(block_index + 1) * SAMPLES_LOCAL]
        rounded = gram(piece).astype(jnp.bfloat16)
        rounded = lax.optimization_barrier(rounded).astype(jnp.float32)
        total = rounded if total is None else total + rounded
    return total


def reference(voltages, assignment, slot_subarray_index):
    rows = result_slot_lookup(assignment, slot_subarray_index)

    def one_channel(block):
        return blocked_gram(compact(block[:, None], rows))[:, 0]

    result = lax.map(one_channel, jnp.moveaxis(voltages, 1, 0))
    return jnp.transpose(result, (1, 0, 2, 3, 4))
```

```python
import jax
import jax.numpy as jnp
from jax import lax
from jax.experimental import pallas as pl
from jax.experimental.pallas import tpu as pltpu
from jax.sharding import PartitionSpec as P

SLOT = 384
LANES = 128
MESH = pl.DeviceIdType.MESH


def partner(me, step, count):
    if count & (count - 1):
        raise ValueError("axis size")
    other = me
    bit = 1
    while bit < count:
        if step & bit:
            other = other + bit - 2 * bit * (lax.div(me, bit) % 2)
        bit *= 2
    return other


def place_of_inputs(owner_ref, slots_ref, subarrays, slot):
    owner = owner_ref[...]
    rows = owner.shape[0]
    member = [(owner == slots_ref[s]).astype(jnp.float32) for s in range(subarrays)]
    stacked = jnp.concatenate(member, axis=0).astype(jnp.bfloat16)
    a = lax.broadcasted_iota(jnp.int32, (LANES, LANES), 0)
    b = lax.broadcasted_iota(jnp.int32, (LANES, LANES), 1)
    before = (a < b).astype(jnp.float32).astype(jnp.bfloat16)
    within = jnp.dot(stacked, before, preferred_element_type=jnp.float32)
    totals = jnp.dot(
        stacked, jnp.ones((LANES, LANES), jnp.bfloat16), preferred_element_type=jnp.float32
    ).astype(jnp.bfloat16)
    size = subarrays * rows
    c = lax.broadcasted_iota(jnp.int32, (size, size), 0)
    d = lax.broadcasted_iota(jnp.int32, (size, size), 1)
    earlier = ((c // rows == d // rows) & (d < c)).astype(jnp.float32).astype(jnp.bfloat16)
    rank = within + jnp.dot(earlier, totals, preferred_element_type=jnp.float32)
    half = jnp.zeros(owner.shape, jnp.float32)
    for s in range(subarrays):
        half = half + member[s] * (rank[s * rows : (s + 1) * rows] + float(s * (slot // 2)))
    high = jnp.floor(half * (1.0 / 64.0))
    low = half - high * 64.0
    e = lax.broadcasted_iota(jnp.int32, (LANES, 2 * LANES), 0)
    f = lax.broadcasted_iota(jnp.int32, (LANES, 2 * LANES), 1)
    spread = (f // 2 == e).astype(jnp.float32).astype(jnp.bfloat16)
    wide = jnp.dot(
        jnp.concatenate([high, low], axis=0).astype(jnp.bfloat16),
        spread,
        preferred_element_type=jnp.float32,
    )
    odd = (lax.broadcasted_iota(jnp.int32, (rows, 2 * LANES), 1) % 2).astype(jnp.float32)
    return 2.0 * (64.0 * wide[:rows] + wide[rows:]) + odd


def make_exchange(chans, groups, subarrays, slot, inputs, local, samples):
    held = subarrays // groups
    block = held * slot
    chan_steps = list(range(chans - 1, 0, -1))
    tm_steps = [s for s in range(groups // 2, groups)] + [s for s in range(1, groups // 2)]

    def kernel(
        volt_ref, owner_ref, slots_ref, out_ref,
        mine, arrived, pick, packed, load_sem, own_sem, csend, crecv, tsend, trecv,
    ):
        chan = lax.axis_index("chan")
        tm = lax.axis_index("tm")
        chan_peers = {s: partner(chan, s, chans) for s in chan_steps}
        tm_peers = {s: partner(tm, s, groups) for s in tm_steps}
        loads = []
        for k in range(2):
            copy = pltpu.make_async_copy(volt_ref.at[k], mine.at[k], load_sem.at[k])
            copy.start()
            loads.append(copy)
        barrier = pltpu.get_barrier_semaphore()
        for s in tm_steps:
            pl.semaphore_signal(barrier, inc=1, device_id={"tm": tm_peers[s]}, device_id_type=MESH)
        for s in chan_steps:
            pl.semaphore_signal(barrier, inc=1, device_id={"chan": chan_peers[s]}, device_id_type=MESH)
        for load in loads:
            load.wait()
        pl.semaphore_wait(barrier, len(tm_steps) + len(chan_steps))

        here = pl.ds(pl.multiple_of(chan * local, local), local)
        sent = []
        for k in range(2):
            copies = []
            for s in chan_steps:
                copy = pltpu.make_async_remote_copy(
                    src_ref=mine.at[k, chan_peers[s]],
                    dst_ref=arrived.at[k, here],
                    send_sem=csend.at[k, s],
                    recv_sem=crecv.at[k, s],
                    device_id={"chan": chan_peers[s]},
                    device_id_type=MESH,
                )
                copy.start()
                copies.append(copy)
            own = pltpu.make_async_copy(mine.at[k, chan], arrived.at[k, here], own_sem.at[k])
            own.start()
            sent.append((own, copies))

        place = place_of_inputs(owner_ref, slots_ref, subarrays, slot)
        width = 2 * LANES
        order = tm_steps + [0]
        for i, s in enumerate(order):
            holder = tm_peers[s] if s else tm
            first = (holder * block).astype(jnp.float32)
            iota = lax.broadcasted_iota(jnp.int32, (block, width), 0).astype(jnp.float32)
            for r in range(inputs // width):
                hit = iota == (place[r : r + 1] - first)
                pick[i, :, r * width : (r + 1) * width] = jnp.where(hit, 1.0, 0.0).astype(jnp.bfloat16)

        onward = []
        for k in range(2):
            own, copies = sent[k]
            own.wait()
            for copy in copies:
                copy.wait_recv()
            for i, s in enumerate(order):
                rows = jnp.dot(pick[i], arrived[k], preferred_element_type=jnp.float32)
                rows = rows.astype(jnp.bfloat16).reshape(held, slot, samples)
                if s == 0:
                    out_ref[:, k, pl.ds(tm, 1)] = rows[:, None]
                    continue
                packed[k, i] = rows
                copy = pltpu.make_async_remote_copy(
                    src_ref=packed.at[k, i],
                    dst_ref=out_ref.at[:, k, tm],
                    send_sem=tsend.at[k, s],
                    recv_sem=trecv.at[k, s],
                    device_id={"tm": tm_peers[s]},
                    device_id_type=MESH,
                )
                copy.start()
                onward.append(copy)
        for _, copies in sent:
            for copy in copies:
                copy.wait_send()
        for copy in onward:
            copy.wait()

    return pl.pallas_call(
        kernel,
        out_shape=jax.ShapeDtypeStruct((held, 2, groups, slot, samples), jnp.bfloat16),
        in_specs=[
            pl.BlockSpec(memory_space=pl.ANY),
            pl.BlockSpec(memory_space=pltpu.VMEM),
            pl.BlockSpec(memory_space=pltpu.SMEM),
        ],
        out_specs=pl.BlockSpec(memory_space=pltpu.VMEM),
        scratch_shapes=[
            pltpu.VMEM((2, chans, local, samples), jnp.bfloat16),
            pltpu.VMEM((2, inputs, samples), jnp.bfloat16),
            pltpu.VMEM((groups, block, inputs), jnp.bfloat16),
            pltpu.VMEM((2, groups - 1, held, slot, samples), jnp.bfloat16),
            pltpu.SemaphoreType.DMA((2,)),
            pltpu.SemaphoreType.DMA((2,)),
            pltpu.SemaphoreType.DMA((2, chans)),
            pltpu.SemaphoreType.DMA((2, chans)),
            pltpu.SemaphoreType.DMA((2, groups)),
            pltpu.SemaphoreType.DMA((2, groups)),
        ],
        compiler_params=pltpu.CompilerParams(
            collective_id=0, has_side_effects=True, vmem_limit_bytes=48 * 2**20
        ),
        name="exchange",
    )


def make_gram(groups, held, slot, samples):
    tile = 128
    tiles = slot // tile

    def kernel(x_ref, out_ref, stage, sems):
        copies = []
        for s in range(held):
            right = jnp.concatenate([x_ref[s, k, g] for g in range(groups) for k in range(2)], axis=-1)
            for part in range(2):
                for t in range(tiles):
                    rows = pl.ds(t * tile, tile)
                    if part == 0:
                        pieces = [x_ref[s, k, g, rows] for g in range(groups) for k in range(2)]
                    else:
                        pieces = [
                            x_ref[s, 1, g, rows] if k == 0 else -x_ref[s, 0, g, rows]
                            for g in range(groups) for k in range(2)
                        ]
                    left = jnp.concatenate(pieces, axis=-1)
                    stage[s, part, rows] = lax.dot_general(
                        left, right, (((1,), (1,)), ((), ())), preferred_element_type=jnp.float32
                    )
                    copy = pltpu.make_async_copy(
                        stage.at[s, part, rows], out_ref.at[s, 0, part, rows], sems.at[s, part, t]
                    )
                    copy.start()
                    copies.append(copy)
        for copy in copies:
            copy.wait()

    return pl.pallas_call(
        kernel,
        out_shape=jax.ShapeDtypeStruct((held, 1, 2, slot, slot), jnp.float32),
        in_specs=[pl.BlockSpec(memory_space=pltpu.VMEM)],
        out_specs=pl.BlockSpec(memory_space=pl.ANY),
        scratch_shapes=[
            pltpu.VMEM((held, 2, slot, slot), jnp.float32),
            pltpu.SemaphoreType.DMA((held, 2, tiles)),
        ],
        name="gram",
    )


def shards(voltages, assignment, slot_subarray_index):
    _, chans, local, samples = voltages.shape
    subarrays = slot_subarray_index.shape[0]
    antennas = assignment.shape[0]
    groups = lax.axis_size("tm")
    exchange = make_exchange(chans, groups, subarrays, SLOT, 2 * antennas, local, samples)
    owner = assignment.reshape(antennas // LANES, LANES)
    gathered = exchange(voltages, owner, slot_subarray_index)
    return make_gram(groups, subarrays // groups, SLOT, samples)(gathered)


def solution(mesh):
    placed = (P(None, None, "chan", "tm"), P(), P())
    return jax.shard_map(
        shards,
        mesh=mesh,
        in_specs=placed,
        out_specs=P("tm", "chan", None, None, None),
        check_vma=False,
    )
```

```python
import jax
import jax.numpy as jnp
from jax import lax
from jax.experimental import pallas as pl
from jax.experimental.pallas import tpu as pltpu
from jax.sharding import PartitionSpec as P

SLOT = 384
LANES = 128
MESH = pl.DeviceIdType.MESH


def partner(me, step, count):
    if count & (count - 1):
        raise ValueError("axis size")
    other = me
    bit = 1
    while bit < count:
        if step & bit:
            other = other + bit - 2 * bit * (lax.div(me, bit) % 2)
        bit *= 2
    return other


def place_of_inputs(owner_ref, slots_ref, subarrays, slot):
    owner = owner_ref[...]
    rows = owner.shape[0]
    member = [(owner == slots_ref[s]).astype(jnp.float32) for s in range(subarrays)]
    stacked = jnp.concatenate(member, axis=0).astype(jnp.bfloat16)
    a = lax.broadcasted_iota(jnp.int32, (LANES, LANES), 0)
    b = lax.broadcasted_iota(jnp.int32, (LANES, LANES), 1)
    before = (a < b).astype(jnp.float32).astype(jnp.bfloat16)
    within = jnp.dot(stacked, before, preferred_element_type=jnp.float32)
    totals = jnp.dot(
        stacked, jnp.ones((LANES, LANES), jnp.bfloat16), preferred_element_type=jnp.float32
    ).astype(jnp.bfloat16)
    size = subarrays * rows
    c = lax.broadcasted_iota(jnp.int32, (size, size), 0)
    d = lax.broadcasted_iota(jnp.int32, (size, size), 1)
    earlier = ((c // rows == d // rows) & (d < c)).astype(jnp.float32).astype(jnp.bfloat16)
    rank = within + jnp.dot(earlier, totals, preferred_element_type=jnp.float32)
    half = jnp.zeros(owner.shape, jnp.float32)
    for s in range(subarrays):
        half = half + member[s] * (rank[s * rows : (s + 1) * rows] + float(s * (slot // 2)))
    high = jnp.floor(half * (1.0 / 64.0))
    low = half - high * 64.0
    e = lax.broadcasted_iota(jnp.int32, (LANES, 2 * LANES), 0)
    f = lax.broadcasted_iota(jnp.int32, (LANES, 2 * LANES), 1)
    spread = (f // 2 == e).astype(jnp.float32).astype(jnp.bfloat16)
    wide = jnp.dot(
        jnp.concatenate([high, low], axis=0).astype(jnp.bfloat16),
        spread,
        preferred_element_type=jnp.float32,
    )
    odd = (lax.broadcasted_iota(jnp.int32, (rows, 2 * LANES), 1) % 2).astype(jnp.float32)
    return 2.0 * (64.0 * wide[:rows] + wide[rows:]) + odd


def flip(me, mask, count):
    out = me * 0
    bit = 1
    while bit < count:
        out = out + bit * ((lax.div(me, bit) + lax.div(mask, bit)) % 2)
        bit *= 2
    return out


def line_order(tm, groups):
    if groups != 4:
        masks = [tm * 0 + s for s in range(1, groups)]
        return masks, masks
    inner = lax.div(tm + 1, 2) % 2
    return [1 + inner, 2 + inner, 3 - 2 * inner], [tm * 0 + 1, 2 + inner, 3 - inner]


def make_correlator(chans, groups, subarrays, slot, antennas, local, samples):
    held = subarrays // groups
    block = held * slot
    inputs = 2 * antennas
    width = 2 * LANES
    chan_steps = list(range(chans - 1, 0, -1))

    def kernel(
        volt_hbm, owner_hbm, slots_hbm, out_ref,
        mine, arrived, pick, packed, taken, owner_ref, slots_ref,
        load_sem, own_sem, csend, crecv, tsend, trecv,
    ):
        chan = lax.axis_index("chan")
        tm = lax.axis_index("tm")
        chan_peers = {s: partner(chan, s, chans) for s in chan_steps}
        send_masks, recv_masks = line_order(tm, groups)
        tm_peers = [flip(tm, m, groups) for m in send_masks]

        loads = [
            pltpu.make_async_copy(volt_hbm.at[0], mine.at[0], load_sem.at[0]),
            pltpu.make_async_copy(slots_hbm, slots_ref, load_sem.at[2]),
            pltpu.make_async_copy(owner_hbm, owner_ref, load_sem.at[3]),
            pltpu.make_async_copy(volt_hbm.at[1], mine.at[1], load_sem.at[1]),
        ]
        for load in loads:
            load.start()
        barrier = pltpu.get_barrier_semaphore()
        for peer in tm_peers:
            pl.semaphore_signal(barrier, inc=1, device_id={"tm": peer}, device_id_type=MESH)
        for s in chan_steps:
            pl.semaphore_signal(barrier, inc=1, device_id={"chan": chan_peers[s]}, device_id_type=MESH)
        for load in loads:
            load.wait()
        pl.semaphore_wait(barrier, len(tm_peers) + len(chan_steps))

        here = pl.ds(pl.multiple_of(chan * local, local), local)

        def swap_channels(k):
            copies = []
            for s in chan_steps:
                copy = pltpu.make_async_remote_copy(
                    src_ref=mine.at[k, chan_peers[s]],
                    dst_ref=arrived.at[k, here],
                    send_sem=csend.at[k, s],
                    recv_sem=crecv.at[k, s],
                    device_id={"chan": chan_peers[s]},
                    device_id_type=MESH,
                )
                copy.start()
                copies.append(copy)
            own = pltpu.make_async_copy(mine.at[k, chan], arrived.at[k, here], own_sem.at[k])
            own.start()
            return own, copies

        swaps = [swap_channels(0), None]

        place = place_of_inputs(owner_ref, slots_ref, subarrays, slot)
        iota = lax.broadcasted_iota(jnp.int32, (block, width), 0).astype(jnp.float32)
        for i, holder in enumerate(tm_peers + [tm]):
            first = (holder * block).astype(jnp.float32)
            for r in range(inputs // width):
                hit = iota == (place[r : r + 1] - first)
                pick[i, :, r * width : (r + 1) * width] = jnp.where(hit, 1.0, 0.0).astype(jnp.bfloat16)

        onward = []
        for k in range(2):
            own, copies = swaps[k]
            own.wait()
            for copy in copies:
                copy.wait_recv()
            if k == 0:
                swaps[1] = swap_channels(1)
            for i, peer in enumerate(tm_peers + [tm]):
                rows = jnp.dot(pick[i], arrived[k], preferred_element_type=jnp.float32)
                rows = rows.astype(jnp.bfloat16).reshape(held, slot, samples)
                if i == groups - 1:
                    taken[:, k, pl.ds(tm, 1)] = rows[:, None]
                    continue
                packed[k, i] = rows
                copy = pltpu.make_async_remote_copy(
                    src_ref=packed.at[k, i],
                    dst_ref=taken.at[:, k, tm],
                    send_sem=tsend.at[k, send_masks[i]],
                    recv_sem=trecv.at[k, send_masks[i]],
                    device_id={"tm": peer},
                    device_id_type=MESH,
                )
                copy.start()
                onward.append(copy)

        def add_block(group, fresh):
            for s in range(held):
                re = taken[s, 0, group]
                im = taken[s, 1, group]
                right = jnp.concatenate([re, im], axis=-1)
                for part, left in ((0, right), (1, jnp.concatenate([im, -re], axis=-1))):
                    term = lax.dot_general(
                        left, right, (((1,), (1,)), ((), ())), preferred_element_type=jnp.float32
                    )
                    if fresh:
                        out_ref[s, 0, part] = term
                    else:
                        out_ref[s, 0, part] += term

        add_block(tm, True)
        for mask in recv_masks:
            peer = flip(tm, mask, groups)
            for k in range(2):
                pltpu.make_async_remote_copy(
                    src_ref=packed.at[k, 0],
                    dst_ref=taken.at[:, k, peer],
                    send_sem=tsend.at[k, mask],
                    recv_sem=trecv.at[k, mask],
                    device_id={"tm": peer},
                    device_id_type=MESH,
                ).wait_recv()
            add_block(peer, False)
        for _, copies in swaps:
            for copy in copies:
                copy.wait_send()
        for copy in onward:
            copy.wait_send()

    return pl.pallas_call(
        kernel,
        out_shape=jax.ShapeDtypeStruct((held, 1, 2, slot, slot), jnp.float32),
        in_specs=[pl.BlockSpec(memory_space=pltpu.HBM)] * 3,
        out_specs=pl.BlockSpec(memory_space=pltpu.VMEM),
        scratch_shapes=[
            pltpu.VMEM((2, chans, local, samples), jnp.bfloat16),
            pltpu.VMEM((2, inputs, samples), jnp.bfloat16),
            pltpu.VMEM((groups, block, inputs), jnp.bfloat16),
            pltpu.VMEM((2, groups - 1, held, slot, samples), jnp.bfloat16),
            pltpu.VMEM((held, 2, groups, slot, samples), jnp.bfloat16),
            pltpu.VMEM((antennas // LANES, LANES), jnp.int32),
            pltpu.SMEM((subarrays,), jnp.int32),
            pltpu.SemaphoreType.DMA((4,)),
            pltpu.SemaphoreType.DMA((2,)),
            pltpu.SemaphoreType.DMA((2, chans)),
            pltpu.SemaphoreType.DMA((2, chans)),
            pltpu.SemaphoreType.DMA((2, groups)),
            pltpu.SemaphoreType.DMA((2, groups)),
        ],
        compiler_params=pltpu.CompilerParams(
            collective_id=0, has_side_effects=True, vmem_limit_bytes=61 * 2**20
        ),
        name="correlate",
    )


def shards(voltages, assignment, slot_subarray_index):
    _, chans, local, samples = voltages.shape
    subarrays = slot_subarray_index.shape[0]
    antennas = assignment.shape[0]
    groups = lax.axis_size("tm")
    correlate = make_correlator(chans, groups, subarrays, SLOT, antennas, local, samples)
    return correlate(voltages, assignment.reshape(antennas // LANES, LANES), slot_subarray_index)


def solution(mesh):
    placed = (P(None, None, "chan", "tm"), P(), P())
    return jax.shard_map(
        shards,
        mesh=mesh,
        in_specs=placed,
        out_specs=P("tm", "chan", None, None, None),
        check_vma=False,
    )
```

```python
import jax
import jax.numpy as jnp
from jax import lax
from jax.experimental import pallas as pl
from jax.experimental.pallas import tpu as pltpu
from jax.sharding import PartitionSpec as P

SLOT = 384
LANES = 128
MESH = pl.DeviceIdType.MESH


def partner(me, step, count):
    if count & (count - 1):
        raise ValueError("axis size")
    other = me
    bit = 1
    while bit < count:
        if step & bit:
            other = other + bit - 2 * bit * (lax.div(me, bit) % 2)
        bit *= 2
    return other


def place_of_inputs(owner_ref, slots_ref, subarrays, slot):
    owner = owner_ref[...]
    rows = owner.shape[0]
    member = [(owner == slots_ref[s]).astype(jnp.float32) for s in range(subarrays)]
    stacked = jnp.concatenate(member, axis=0).astype(jnp.bfloat16)
    a = lax.broadcasted_iota(jnp.int32, (LANES, LANES), 0)
    b = lax.broadcasted_iota(jnp.int32, (LANES, LANES), 1)
    before = (a < b).astype(jnp.float32).astype(jnp.bfloat16)
    within = jnp.dot(stacked, before, preferred_element_type=jnp.float32)
    totals = jnp.dot(
        stacked, jnp.ones((LANES, LANES), jnp.bfloat16), preferred_element_type=jnp.float32
    ).astype(jnp.bfloat16)
    size = subarrays * rows
    c = lax.broadcasted_iota(jnp.int32, (size, size), 0)
    d = lax.broadcasted_iota(jnp.int32, (size, size), 1)
    earlier = ((c // rows == d // rows) & (d < c)).astype(jnp.float32).astype(jnp.bfloat16)
    rank = within + jnp.dot(earlier, totals, preferred_element_type=jnp.float32)
    half = jnp.zeros(owner.shape, jnp.float32)
    for s in range(subarrays):
        half = half + member[s] * (rank[s * rows : (s + 1) * rows] + float(s * (slot // 2)))
    high = jnp.floor(half * (1.0 / 64.0))
    low = half - high * 64.0
    e = lax.broadcasted_iota(jnp.int32, (LANES, 2 * LANES), 0)
    f = lax.broadcasted_iota(jnp.int32, (LANES, 2 * LANES), 1)
    spread = (f // 2 == e).astype(jnp.float32).astype(jnp.bfloat16)
    wide = jnp.dot(
        jnp.concatenate([high, low], axis=0).astype(jnp.bfloat16),
        spread,
        preferred_element_type=jnp.float32,
    )
    odd = (lax.broadcasted_iota(jnp.int32, (rows, 2 * LANES), 1) % 2).astype(jnp.float32)
    return 2.0 * (64.0 * wide[:rows] + wide[rows:]) + odd


def flip(me, mask, count):
    out = me * 0
    bit = 1
    while bit < count:
        out = out + bit * ((lax.div(me, bit) + lax.div(mask, bit)) % 2)
        bit *= 2
    return out


def line_order(tm, groups):
    if groups != 4:
        masks = [tm * 0 + s for s in range(1, groups)]
        return masks, masks
    inner = lax.div(tm + 1, 2) % 2
    return [1 + inner, 2 + inner, 3 - 2 * inner], [tm * 0 + 1, 2 + inner, 3 - inner]


def make_correlator(chans, groups, subarrays, slot, antennas, local, samples):
    held = subarrays // groups
    block = held * slot
    inputs = 2 * antennas
    width = 2 * LANES
    chan_steps = list(range(chans - 1, 0, -1))

    def kernel(
        volt_hbm, owner_hbm, slots_hbm, out_ref,
        mine, arrived, pick, packed, taken, owner_ref, slots_ref,
        load_sem, own_sem, csend, crecv, tsend, trecv,
    ):
        chan = lax.axis_index("chan")
        tm = lax.axis_index("tm")
        chan_peers = {s: partner(chan, s, chans) for s in chan_steps}
        send_masks, recv_masks = line_order(tm, groups)
        tm_peers = [flip(tm, m, groups) for m in send_masks]

        loads = [
            pltpu.make_async_copy(volt_hbm.at[0], mine.at[0], load_sem.at[0]),
            pltpu.make_async_copy(slots_hbm, slots_ref, load_sem.at[2]),
            pltpu.make_async_copy(owner_hbm, owner_ref, load_sem.at[3]),
            pltpu.make_async_copy(volt_hbm.at[1], mine.at[1], load_sem.at[1]),
        ]
        for load in loads:
            load.start()
        barrier = pltpu.get_barrier_semaphore()
        for peer in tm_peers:
            pl.semaphore_signal(barrier, inc=1, device_id={"tm": peer}, device_id_type=MESH)
        for s in chan_steps:
            pl.semaphore_signal(barrier, inc=1, device_id={"chan": chan_peers[s]}, device_id_type=MESH)
        for load in loads:
            load.wait()
        pl.semaphore_wait(barrier, len(tm_peers) + len(chan_steps))

        here = pl.ds(pl.multiple_of(chan * local, local), local)

        def swap_channels(k):
            copies = []
            for s in chan_steps:
                copy = pltpu.make_async_remote_copy(
                    src_ref=mine.at[k, chan_peers[s]],
                    dst_ref=arrived.at[k, here],
                    send_sem=csend.at[k, s],
                    recv_sem=crecv.at[k, s],
                    device_id={"chan": chan_peers[s]},
                    device_id_type=MESH,
                )
                copy.start()
                copies.append(copy)
            own = pltpu.make_async_copy(mine.at[k, chan], arrived.at[k, here], own_sem.at[k])
            own.start()
            return own, copies

        swaps = [swap_channels(0), None]

        place = place_of_inputs(owner_ref, slots_ref, subarrays, slot)
        iota = lax.broadcasted_iota(jnp.int32, (block, width), 0).astype(jnp.float32)
        for i, holder in enumerate(tm_peers + [tm]):
            first = (holder * block).astype(jnp.float32)
            for r in range(inputs // width):
                hit = iota == (place[r : r + 1] - first)
                pick[i, :, r * width : (r + 1) * width] = jnp.where(hit, 1.0, 0.0).astype(jnp.bfloat16)

        onward = []
        for k in range(2):
            own, copies = swaps[k]
            own.wait()
            for copy in copies:
                copy.wait_recv()
            if k == 0:
                swaps[1] = swap_channels(1)
            for i, peer in enumerate(tm_peers + [tm]):
                rows = jnp.dot(pick[i], arrived[k], preferred_element_type=jnp.float32)
                rows = rows.astype(jnp.bfloat16).reshape(held, slot, samples)
                if i == groups - 1:
                    taken[:, k, pl.ds(tm, 1)] = rows[:, None]
                    continue
                packed[k, i] = rows
                copy = pltpu.make_async_remote_copy(
                    src_ref=packed.at[k, i],
                    dst_ref=taken.at[:, k, tm],
                    send_sem=tsend.at[k, send_masks[i]],
                    recv_sem=trecv.at[k, send_masks[i]],
                    device_id={"tm": peer},
                    device_id_type=MESH,
                )
                copy.start()
                onward.append(copy)

        def add_block(group, fresh):
            for s in range(held):
                re = taken[s, 0, group]
                im = taken[s, 1, group]
                right = jnp.concatenate([re, im], axis=-1)
                for part, left in ((0, right), (1, jnp.concatenate([im, -re], axis=-1))):
                    term = lax.dot_general(
                        left, right, (((1,), (1,)), ((), ())), preferred_element_type=jnp.float32
                    )
                    if fresh:
                        out_ref[s, 0, part] = term
                    else:
                        out_ref[s, 0, part] += term

        add_block(tm, True)
        for mask in recv_masks:
            peer = flip(tm, mask, groups)
            for k in range(2):
                pltpu.make_async_remote_copy(
                    src_ref=packed.at[k, 0],
                    dst_ref=taken.at[:, k, peer],
                    send_sem=tsend.at[k, mask],
                    recv_sem=trecv.at[k, mask],
                    device_id={"tm": peer},
                    device_id_type=MESH,
                ).wait_recv()
            add_block(peer, False)
        for _, copies in swaps:
            for copy in copies:
                copy.wait_send()
        for copy in onward:
            copy.wait_send()

    return pl.pallas_call(
        kernel,
        out_shape=jax.ShapeDtypeStruct((held, 1, 2, slot, slot), jnp.float32),
        in_specs=[pl.BlockSpec(memory_space=pltpu.HBM)] * 3,
        out_specs=pl.BlockSpec(memory_space=pltpu.VMEM),
        scratch_shapes=[
            pltpu.VMEM((2, chans, local, samples), jnp.bfloat16),
            pltpu.VMEM((2, inputs, samples), jnp.bfloat16),
            pltpu.VMEM((groups, block, inputs), jnp.bfloat16),
            pltpu.VMEM((2, groups - 1, held, slot, samples), jnp.bfloat16),
            pltpu.VMEM((held, 2, groups, slot, samples), jnp.bfloat16),
            pltpu.VMEM((antennas // LANES, LANES), jnp.int32),
            pltpu.SMEM((subarrays,), jnp.int32),
            pltpu.SemaphoreType.DMA((4,)),
            pltpu.SemaphoreType.DMA((2,)),
            pltpu.SemaphoreType.DMA((2, chans)),
            pltpu.SemaphoreType.DMA((2, chans)),
            pltpu.SemaphoreType.DMA((2, groups)),
            pltpu.SemaphoreType.DMA((2, groups)),
        ],
        compiler_params=pltpu.CompilerParams(
            collective_id=0, has_side_effects=True, vmem_limit_bytes=48 * 2**20
        ),
        name="correlate",
    )


def shards(voltages, assignment, slot_subarray_index):
    _, chans, local, samples = voltages.shape
    subarrays = slot_subarray_index.shape[0]
    antennas = assignment.shape[0]
    groups = lax.axis_size("tm")
    correlate = make_correlator(chans, groups, subarrays, SLOT, antennas, local, samples)
    owner = assignment.reshape(antennas // LANES, LANES)
    operands = [pltpu.with_memory_space_constraint(x, pltpu.HBM) for x in (voltages, owner, slot_subarray_index)]
    return correlate(*operands)


def solution(mesh):
    placed = (P(None, None, "chan", "tm"), P(), P())
    return jax.shard_map(
        shards,
        mesh=mesh,
        in_specs=placed,
        out_specs=P("tm", "chan", None, None, None),
        check_vma=False,
    )
```

```python
import jax
import jax.numpy as jnp
from jax import lax
from jax.experimental import pallas as pl
from jax.experimental.pallas import tpu as pltpu
from jax.sharding import PartitionSpec as P

SLOT = 384
LANES = 128
MESH = pl.DeviceIdType.MESH


def partner(me, step, count):
    if count & (count - 1):
        raise ValueError("axis size")
    other = me
    bit = 1
    while bit < count:
        if step & bit:
            other = other + bit - 2 * bit * (lax.div(me, bit) % 2)
        bit *= 2
    return other


def place_of_inputs(owner_ref, slots_ref, subarrays, slot):
    owner = owner_ref[...]
    rows = owner.shape[0]
    member = [(owner == slots_ref[s]).astype(jnp.float32) for s in range(subarrays)]
    stacked = jnp.concatenate(member, axis=0).astype(jnp.bfloat16)
    a = lax.broadcasted_iota(jnp.int32, (LANES, LANES), 0)
    b = lax.broadcasted_iota(jnp.int32, (LANES, LANES), 1)
    before = (a < b).astype(jnp.float32).astype(jnp.bfloat16)
    within = jnp.dot(stacked, before, preferred_element_type=jnp.float32)
    totals = jnp.dot(
        stacked, jnp.ones((LANES, LANES), jnp.bfloat16), preferred_element_type=jnp.float32
    ).astype(jnp.bfloat16)
    size = subarrays * rows
    c = lax.broadcasted_iota(jnp.int32, (size, size), 0)
    d = lax.broadcasted_iota(jnp.int32, (size, size), 1)
    earlier = ((c // rows == d // rows) & (d < c)).astype(jnp.float32).astype(jnp.bfloat16)
    rank = within + jnp.dot(earlier, totals, preferred_element_type=jnp.float32)
    half = jnp.zeros(owner.shape, jnp.float32)
    for s in range(subarrays):
        half = half + member[s] * (rank[s * rows : (s + 1) * rows] + float(s * (slot // 2)))
    high = jnp.floor(half * (1.0 / 64.0))
    low = half - high * 64.0
    e = lax.broadcasted_iota(jnp.int32, (LANES, 2 * LANES), 0)
    f = lax.broadcasted_iota(jnp.int32, (LANES, 2 * LANES), 1)
    spread = (f // 2 == e).astype(jnp.float32).astype(jnp.bfloat16)
    wide = jnp.dot(
        jnp.concatenate([high, low], axis=0).astype(jnp.bfloat16),
        spread,
        preferred_element_type=jnp.float32,
    )
    odd = (lax.broadcasted_iota(jnp.int32, (rows, 2 * LANES), 1) % 2).astype(jnp.float32)
    return 2.0 * (64.0 * wide[:rows] + wide[rows:]) + odd


def flip(me, mask, count):
    out = me * 0
    bit = 1
    while bit < count:
        out = out + bit * ((lax.div(me, bit) + lax.div(mask, bit)) % 2)
        bit *= 2
    return out


def line_order(tm, groups):
    if groups != 4:
        masks = [tm * 0 + s for s in range(1, groups)]
        return masks, masks
    inner = lax.div(tm + 1, 2) % 2
    return [1 + inner, 2 + inner, 3 - 2 * inner], [tm * 0 + 1, 2 + inner, 3 - inner]


def make_correlator(chans, groups, subarrays, slot, antennas, local, samples):
    held = subarrays // groups
    block = held * slot
    inputs = 2 * antennas
    width = 2 * LANES
    chan_steps = list(range(chans - 1, 0, -1))

    def kernel(
        volt_hbm, owner_hbm, slots_hbm, out_ref,
        mine, arrived, pick, packed, taken, owner_ref, slots_ref,
        load_sem, own_sem, csend, crecv, tsend, trecv,
    ):
        chan = lax.axis_index("chan")
        tm = lax.axis_index("tm")
        chan_peers = {s: partner(chan, s, chans) for s in chan_steps}
        send_masks, recv_masks = line_order(tm, groups)
        tm_peers = [flip(tm, m, groups) for m in send_masks]

        loads = [
            pltpu.make_async_copy(volt_hbm.at[0], mine.at[0], load_sem.at[0]),
            pltpu.make_async_copy(slots_hbm, slots_ref, load_sem.at[2]),
            pltpu.make_async_copy(owner_hbm, owner_ref, load_sem.at[3]),
            pltpu.make_async_copy(volt_hbm.at[1], mine.at[1], load_sem.at[1]),
        ]
        for load in loads:
            load.start()
        barrier = pltpu.get_barrier_semaphore()
        for peer in tm_peers:
            pl.semaphore_signal(barrier, inc=1, device_id={"tm": peer}, device_id_type=MESH)
        for s in chan_steps:
            pl.semaphore_signal(barrier, inc=1, device_id={"chan": chan_peers[s]}, device_id_type=MESH)
        for load in loads:
            load.wait()
        pl.semaphore_wait(barrier, len(tm_peers) + len(chan_steps))

        here = pl.ds(pl.multiple_of(chan * local, local), local)

        def swap_channels(k):
            copies = []
            for s in chan_steps:
                copy = pltpu.make_async_remote_copy(
                    src_ref=mine.at[k, chan_peers[s]],
                    dst_ref=arrived.at[k, here],
                    send_sem=csend.at[k, s],
                    recv_sem=crecv.at[k, s],
                    device_id={"chan": chan_peers[s]},
                    device_id_type=MESH,
                )
                copy.start()
                copies.append(copy)
            own = pltpu.make_async_copy(mine.at[k, chan], arrived.at[k, here], own_sem.at[k])
            own.start()
            return own, copies

        swaps = [swap_channels(0), None]

        place = place_of_inputs(owner_ref, slots_ref, subarrays, slot)
        iota = lax.broadcasted_iota(jnp.int32, (block, width), 0).astype(jnp.float32)
        for i, holder in enumerate(tm_peers + [tm]):
            first = (holder * block).astype(jnp.float32)
            for r in range(inputs // width):
                hit = iota == (place[r : r + 1] - first)
                pick[i, :, r * width : (r + 1) * width] = jnp.where(hit, 1.0, 0.0).astype(jnp.bfloat16)

        onward = []
        for k in range(2):
            own, copies = swaps[k]
            own.wait()
            for copy in copies:
                copy.wait_recv()
            if k == 0:
                swaps[1] = swap_channels(1)
            for i, peer in enumerate(tm_peers + [tm]):
                for h in range(held):
                    rows = jnp.dot(
                        pick[i, h * slot : (h + 1) * slot], arrived[k], preferred_element_type=jnp.float32
                    ).astype(jnp.bfloat16)
                    if i == groups - 1:
                        taken[h, k, tm] = rows
                        continue
                    packed[k, i, h] = rows
                    copy = pltpu.make_async_remote_copy(
                        src_ref=packed.at[k, i, h],
                        dst_ref=taken.at[h, k, tm],
                        send_sem=tsend.at[k, h, send_masks[i]],
                        recv_sem=trecv.at[k, h, send_masks[i]],
                        device_id={"tm": peer},
                        device_id_type=MESH,
                    )
                    copy.start()
                    onward.append(copy)

        def add_block(group, s, fresh):
            re = taken[s, 0, group]
            im = taken[s, 1, group]
            right = jnp.concatenate([re, im], axis=-1)
            for part, left in ((0, right), (1, jnp.concatenate([im, -re], axis=-1))):
                term = lax.dot_general(
                    left, right, (((1,), (1,)), ((), ())), preferred_element_type=jnp.float32
                )
                if fresh:
                    out_ref[s, 0, part] = term
                else:
                    out_ref[s, 0, part] += term

        for h in range(held):
            add_block(tm, h, True)
        for mask in recv_masks:
            peer = flip(tm, mask, groups)
            for h in range(held):
                for k in range(2):
                    pltpu.make_async_remote_copy(
                        src_ref=packed.at[k, 0, h],
                        dst_ref=taken.at[h, k, peer],
                        send_sem=tsend.at[k, h, mask],
                        recv_sem=trecv.at[k, h, mask],
                        device_id={"tm": peer},
                        device_id_type=MESH,
                    ).wait_recv()
                add_block(peer, h, False)
        for _, copies in swaps:
            for copy in copies:
                copy.wait_send()
        for copy in onward:
            copy.wait_send()

    return pl.pallas_call(
        kernel,
        out_shape=jax.ShapeDtypeStruct((held, 1, 2, slot, slot), jnp.float32),
        in_specs=[pl.BlockSpec(memory_space=pltpu.HBM)] * 3,
        out_specs=pl.BlockSpec(memory_space=pltpu.VMEM),
        scratch_shapes=[
            pltpu.VMEM((2, chans, local, samples), jnp.bfloat16),
            pltpu.VMEM((2, inputs, samples), jnp.bfloat16),
            pltpu.VMEM((groups, block, inputs), jnp.bfloat16),
            pltpu.VMEM((2, groups - 1, held, slot, samples), jnp.bfloat16),
            pltpu.VMEM((held, 2, groups, slot, samples), jnp.bfloat16),
            pltpu.VMEM((antennas // LANES, LANES), jnp.int32),
            pltpu.SMEM((subarrays,), jnp.int32),
            pltpu.SemaphoreType.DMA((4,)),
            pltpu.SemaphoreType.DMA((2,)),
            pltpu.SemaphoreType.DMA((2, chans)),
            pltpu.SemaphoreType.DMA((2, chans)),
            pltpu.SemaphoreType.DMA((2, held, groups)),
            pltpu.SemaphoreType.DMA((2, held, groups)),
        ],
        compiler_params=pltpu.CompilerParams(
            collective_id=0, has_side_effects=True, vmem_limit_bytes=48 * 2**20
        ),
        name="correlate",
    )


def shards(voltages, assignment, slot_subarray_index):
    _, chans, local, samples = voltages.shape
    subarrays = slot_subarray_index.shape[0]
    antennas = assignment.shape[0]
    groups = lax.axis_size("tm")
    correlate = make_correlator(chans, groups, subarrays, SLOT, antennas, local, samples)
    owner = assignment.reshape(antennas // LANES, LANES)
    operands = [pltpu.with_memory_space_constraint(x, pltpu.HBM) for x in (voltages, owner, slot_subarray_index)]
    return correlate(*operands)


def solution(mesh):
    placed = (P(None, None, "chan", "tm"), P(), P())
    return jax.shard_map(
        shards,
        mesh=mesh,
        in_specs=placed,
        out_specs=P("tm", "chan", None, None, None),
        check_vma=False,
    )
```
